128 devices in a mesh: col: 16 (over z, y), row: 8 (over x, core).
Axes of the slice: x: 4, y: 4, z: 4, core: 2. Of those that a mesh axis runs over, the one named last changes fastest.
Arguments:
- t_amp: float32 [1024, 20736], P('row', 'col')
- d_denom: float32 [1024, 20736], P('row', 'col')
- v_oovv: bfloat16 [1024, 20736], P('row', 'col')
- v_vvvv: bfloat16 [20736, 20736], P('row', 'col')
- v_oooo: bfloat16 [1024, 1024], replicated
- w_ovov: bfloat16 [4608, 4608], P(None, 'col')
Outputs:
- output: float32 [4608, 4608], P('row', 'col')
All inputs are finite; a program needn't handle non-finite values.
Results may differ from the reference program's by a relative error of at most 0.001.
Values are sent between devices in bfloat16 or wider.
A program may use at most 1 GiB of HBM per device.

```python
import math
import jax
import jax.numpy as jnp
from jax import lax

O = 32
V = 144


def pair_layout(entry_mat):
    entry_four = entry_mat.reshape(O, O, V, V).transpose(0, 2, 1, 3)
    return entry_four.reshape(O * V, O * V)


def setup_inputs(seed: int = 0) -> dict:
    key_list = jax.random.split(jax.random.key(seed), 6)
    amp_scale = 1.5 / math.sqrt(O * V)
    ladder_scale = math.sqrt(O / V)
    hole_scale = math.sqrt(V / O) / 1.5
    t_amp = amp_scale * jax.random.normal(key_list[0], (O * O, V * V), jnp.float32)
    d_denom = -(1.0 + 2.0 * jax.random.uniform(key_list[1], (O * O, V * V), jnp.float32))
    v_oovv = jax.random.normal(key_list[2], (O * O, V * V), jnp.float32).astype(jnp.bfloat16)

    def vvvv_rows(row_block):
        sub_key = jax.random.fold_in(key_list[3], row_block)
        rows_f32 = ladder_scale * jax.random.normal(sub_key, (V, V * V), jnp.float32)
        return rows_f32.astype(jnp.bfloat16)

    v_vvvv = lax.map(vvvv_rows, jnp.arange(V)).reshape(V * V, V * V)
    v_oooo = (hole_scale * jax.random.normal(key_list[4], (O * O, O * O), jnp.float32)).astype(jnp.bfloat16)
    w_ovov = (jax.random.normal(key_list[5], (O * V, O * V), jnp.float32) / 1.5).astype(jnp.bfloat16)
    return {"t_amp": t_amp, "d_denom": d_denom, "v_oovv": v_oovv, "v_vvvv": v_vvvv, "v_oooo": v_oooo, "w_ovov": w_ovov}


def reference(t_amp, d_denom, v_oovv, v_vvvv, v_oooo, w_ovov):
    t_bf = t_amp.astype(jnp.bfloat16)
    r_ladder = jnp.dot(t_bf, v_vvvv, preferred_element_type=jnp.float32)
    x_inter = jnp.dot(v_oovv, t_bf.T, preferred_element_type=jnp.float32)
    w_hole = (v_oooo.astype(jnp.float32) + 0.5 * x_inter).astype(jnp.bfloat16)
    r_hole = jnp.dot(w_hole.T, t_bf, preferred_element_type=jnp.float32)
    entry_sum = v_oovv.astype(jnp.float32) + r_ladder + r_hole
    t_mixed = pair_layout(t_bf)
    r_mixed = jnp.dot(t_mixed, w_ovov, preferred_element_type=jnp.float32)
    return (pair_layout(entry_sum) + r_mixed + r_mixed.T) / pair_layout(d_denom)
```

```python
import functools
import jax
import jax.numpy as jnp
from jax import lax
from jax.experimental import pallas as pl
from jax.experimental.pallas import tpu as pltpu
from jax.sharding import PartitionSpec as P

MESH = pl.DeviceIdType.MESH
F32 = jnp.float32
BF16 = jnp.bfloat16
BLK = 128
NK = 32
ROWS, COLS = 8, 16
LANES = 128
K_STEP = 4


def lane_tiles(width):
    return [(t, min(LANES, width - LANES * t)) for t in range(-(-width // LANES))]


def sweep_kernel(
    nv,
    t_ref, d_ref, vo_ref, v_hbm, oo_hbm, w_hbm,
    out_ref,
    tc, tl, vv, wt, w2, oo, vrow,
    xs, xr, xs2, xr2, wp, wtr,
    part, pair, hop, fin,
    tf, acc_t, m_send, m_recv, i_recv, iq,
    base, d_send, d_recv, b_send, b_recv, osc, dmat, acc,
    local_sem, x_ss, x_rs, sib_ss, sib_rs, z_ss, z_rs, y_ss, y_rs, f_ss,
    pair_ss, pair_rs, hop_ss, hop_rs, fin_ss, fin_rs,
    xa_ss, xa_rs, xb_ss, xb_rs, w_ss, w_rs, m_ss, m_rs, i_ss, i_rs, d_ss, d_rs, b_ss, b_rs,
):
    row = lax.axis_index("row")
    col = lax.axis_index("col")
    x, k = row // 2, row % 2
    z, y = col // 4, col % 4
    va = nv // 16
    ab = va * nv
    n_w = 2 * nv
    a2 = 2 * va
    cut = (va + 1) // 2 * nv
    halves = [(0, cut), (cut, ab - cut)]
    hrow = ab // 2
    sib = (col, 2 * x + 1 - k)
    finish = []

    def send(src, dst, ss, rs, dev, cond=None):
        cp = pltpu.make_async_remote_copy(
            src_ref=src, dst_ref=dst, send_sem=ss, recv_sem=rs, device_id=dev, device_id_type=MESH)
        if cond is None:
            cp.start()
            finish.append(cp.wait_send)
        else:
            @pl.when(cond)
            def _():
                cp.start()

            def done():
                @pl.when(cond)
                def _():
                    cp.wait_send()
            finish.append(done)

    def arrive(dst, rs):
        pltpu.make_async_remote_copy(
            src_ref=dst, dst_ref=dst, send_sem=rs, recv_sem=rs, device_id=(col, row), device_id_type=MESH
        ).wait_recv()

    loads = [
        pltpu.make_async_copy(v_hbm, vv, local_sem.at[0]),
        pltpu.make_async_copy(w_hbm, wt, local_sem.at[1]),
        pltpu.make_async_copy(
            oo_hbm.at[pl.ds(pl.multiple_of(row * BLK, BLK), BLK), pl.ds(pl.multiple_of(col // 2 * LANES, LANES), LANES)],
            oo, local_sem.at[2]),
    ]
    for cp in loads:
        cp.start()

    barrier = pltpu.get_barrier_semaphore()
    for dlt in range(1, COLS):
        pl.semaphore_signal(barrier, inc=1, device_id=((col + dlt) % COLS, row), device_id_type=MESH)
    for dlt in range(1, 8):
        pl.semaphore_signal(barrier, inc=1, device_id=(col, (row + dlt) % 8), device_id_type=MESH)
    for r2 in range(ROWS):
        for h in range(2):
            pl.semaphore_signal(barrier, inc=1, device_id=(2 * row + h, r2), device_id_type=MESH)
    for s in (1, 3):
        pl.semaphore_signal(barrier, inc=1, device_id=(4 * z + (y + s) % 4, 2 * x + 1 - k), device_id_type=MESH)

    tc[row] = t_ref[...].astype(BF16)
    pl.semaphore_wait(barrier, 15 + 7 + 16 + 2)

    def xdev(s):
        return (col, 2 * ((x + s) % 4) + k)

    def zdev(s):
        return (4 * ((z + s) % 4) + y, row)

    for h, (r0, rn) in enumerate(halves):
        src = tc.at[row, pl.ds(r0, rn), :]
        send(src, src, x_ss.at[0, h], x_rs.at[3, h], xdev(1))
        send(src, src, x_ss.at[1, h], x_rs.at[1, h], xdev(3))
    send(tc.at[row], tc.at[row], sib_ss.at[0], sib_rs.at[0], sib)

    rel = (z - x + 4) % 4
    root = rel == 0
    kap = y // 2
    order = [0, 2, 1, 3]

    def x_step():
        for off, h, s, slot in ((3, 0, 1, 2), (1, 1, 3, 3)):
            xb = (x + off) % 4
            r0, rn = halves[h]
            piece = tc.at[2 * xb + k, pl.ds(r0, rn), :]
            arrive(piece, x_rs.at[off, h])
            send(piece, piece, x_ss.at[slot, h], x_rs.at[2, h], xdev(s))

    def x_rest(off):
        xb = (x + off) % 4
        todo = {3: (1,), 1: (0,), 2: (0, 1)}[off]
        for h in todo:
            r0, rn = halves[h]
            arrive(tc.at[2 * xb + k, pl.ds(r0, rn), :], x_rs.at[off, h])
        src = tc.at[2 * xb + k]
        send(src, src, sib_ss.at[off], sib_rs.at[off], sib)

    def z_send(o):
        off = order[o]
        xb = (x + off) % 4
        for h, (r0, rn) in enumerate(halves):
            src = tc.at[2 * xb + k, pl.ds(r0, rn), :]
            dst = tc.at[8 + xb, pl.ds(r0, rn), :]
            send(src, dst, z_ss.at[o, h], z_rs.at[o, h], zdev(1), root)
        for h, (r0, rn) in reversed(list(enumerate(halves))):
            src = tc.at[2 * xb + k, pl.ds(r0, rn), :]
            dst = tc.at[8 + xb, pl.ds(r0, rn), :]
            send(src, dst, z_ss.at[o, 2 + h], z_rs.at[o, h], zdev(3), root)

    def z_wait(o):
        off = order[o]
        xb = (x + off) % 4
        for h, (r0, rn) in enumerate(halves):
            dst = tc.at[8 + xb, pl.ds(r0, rn), :]

            @pl.when(rel != 0)
            def _():
                arrive(dst, z_rs.at[o, h])
            near, s = ((1, 1), (3, 3))[h]
            send(dst, dst, z_ss.at[o, 4], z_rs.at[o, h], zdev(s), rel == near)

    def z_step(o):
        z_send(o)
        z_wait(o)

    def both(p, q):
        return q if p is None else jnp.logical_and(p, q)

    sel_root = jnp.where(root, 1, 0)

    def y_step(o, cond=None):
        off = order[o]
        xb = (x + off) % 4
        blk = sel_root * (2 * xb + k) + (1 - sel_root) * (8 + xb)
        lanes = pl.ds(pl.multiple_of(k * LANES, LANES), LANES)
        for h, (r0, rn) in enumerate(halves):
            src = tc.at[blk, pl.ds(r0, rn), :]
            dst = tl.at[xb, pl.ds((y % 2) * ab + r0, rn), lanes]
            for n, s in enumerate((1, 3)):
                send(src, dst, y_ss.at[o, h, n], y_rs.at[o, y % 2, k, h],
                     (4 * z + (y + s) % 4, 2 * x + kap), cond)
            send(src, dst, y_ss.at[o, h, 2], y_rs.at[o, y % 2, k, h], sib, both(cond, kap != k))

        @pl.when(both(cond, kap == k))
        def _():
            tl[xb, pl.ds(pl.multiple_of((y % 2) * ab, 16), ab), lanes] = tc[blk]

    def y_piece(o, s, q, h):
        xb = (x + order[o]) % 4
        r0, rn = halves[h]
        return tl.at[xb, pl.ds(s * ab + r0, rn), pl.ds(pl.multiple_of(q * LANES, LANES), LANES)]

    def y_forward(o):
        for s in range(2):
            dist = (y - (2 * k + s) + 4) % 4
            for q in range(2):
                for near, h, step in ((1, 0, 1), (3, 1, 3)):
                    piece = y_piece(o, s, q, h)

                    @pl.when(dist == near)
                    def _():
                        arrive(piece, y_rs.at[o, s, q, h])
                    send(piece, piece, f_ss.at[o, s, q], y_rs.at[o, s, q, h],
                         (4 * z + (y + step) % 4, row), dist == near)

    def y_rest(o):
        for s in range(2):
            dist = (y - (2 * k + s) + 4) % 4
            for q in range(2):
                for h in range(2):
                    piece = y_piece(o, s, q, h)
                    other = (1, 3)[1 - h]
                    need = jnp.where(dist == other, 1, 0) + jnp.where(dist == 2, 1, 0) + (
                        jnp.where(dist == 0, 1, 0) * jnp.where(k == q, 0, 1))

                    @pl.when(need == 1)
                    def _():
                        arrive(piece, y_rs.at[o, s, q, h])

    def ladder(o):
        off = order[o]
        xb = (x + off) % 4
        prod = jnp.dot(vv[...], tl[xb], preferred_element_type=F32)
        part[o, 0] = prod[:, :LANES]
        part[o, 1] = prod[:, LANES:]
        send(part.at[o, 1 - k], pair.at[o], pair_ss.at[o], pair_rs.at[o], sib)

    def pair_step(o):
        arrive(pair.at[o], pair_rs.at[o])
        part[o, k] = part[o, k] + pair[o]

    def hop_step():
        for n in range(2):
            send(part.at[1, k, pl.ds(n * hrow, hrow), :], hop.at[n], hop_ss.at[n], hop_rs.at[n], xdev(1 + 2 * n))

    def fin_step(o):
        n = o - 2
        arrive(hop.at[n], hop_rs.at[n])
        rows = pl.ds(n * hrow, hrow)
        part[o, k, rows, :] = part[o, k, rows, :] + hop[n]
        send(part.at[o, k], fin.at[n], fin_ss.at[n], fin_rs.at[n], xdev(order[o]))

    def mixed(o):
        off = order[o]
        xb = (x + off) % 4

        def turn(a, carry):
            blk = tl[xb, pl.ds(pl.multiple_of(a * nv, 16), nv), :].astype(F32)
            flip = blk.T
            for t, wd in lane_tiles(nv):
                tf[2 * a + t, :, 0:wd] = flip[:, t * LANES:t * LANES + wd]
            return carry

        lax.fori_loop(0, a2, turn, 0, unroll=2)

        def one(k0, carry):
            prod = 0.0
            for kk in [k0 * K_STEP + n for n in range(K_STEP)]:
                cols = []
                for t, wd in lane_tiles(nv):
                    rows = [tf[2 * a + t, pl.ds(kk, 8, stride=NK), :] for a in range(a2)]
                    cols.append(jnp.concatenate(rows, axis=0)[:, :wd].astype(BF16))
                lhs = jnp.concatenate(cols, axis=1) if len(cols) > 1 else cols[0]
                prod = prod + jnp.dot(
                    lhs, w2[pl.ds(pl.multiple_of(kk * nv, 16), nv), :], preferred_element_type=F32)
            for t, wd in lane_tiles(n_w):
                acc_t[t, :, 0:wd] = acc_t[t, :, 0:wd] + prod[:, t * LANES:t * LANES + wd]
            return carry

        acc_t[...] = jnp.zeros_like(acc_t)
        lax.fori_loop(0, NK // K_STEP, one, 0)
        for q in range(2):
            for ip in range(2):
                for i2 in range(2):
                    for t, wd in lane_tiles(n_w):
                        m_send[o, q, ip, i2 * a2:(i2 + 1) * a2, t * LANES:t * LANES + wd] = acc_t[
                            t, pl.ds(q * 4 + ip * 2 + i2, a2, stride=8), :][:, :wd]
            r2 = 2 * xb + q
            own = r2 == row
            send(m_send.at[o, q], m_recv.at[row], m_ss.at[o, q], m_rs.at[row], (col, r2), jnp.logical_not(own))

            @pl.when(own)
            def _():
                m_recv[row] = m_send[o, q]
            for ip in range(2):
                c2 = 4 * xb + 2 * q + ip
                own = jnp.where(c2 == col, 1, 0) * jnp.where(col // 2 == row, 1, 0) == 1
                src = m_send.at[o, q, ip]
                send(src, i_recv.at[row, col % 2], i_ss.at[o, q, ip], i_rs.at[row, col % 2],
                     (c2, col // 2), jnp.logical_not(own))

                @pl.when(own)
                def _():
                    i_recv[row, col % 2] = m_send[o, q, ip]

    def split_rows(src, dst):
        for c2 in range(COLS):
            for i in range(4):
                for t, wd in lane_tiles(ab):
                    dst[c2, t, 2 * i:2 * i + 2, 0:wd] = src[i * NK + 2 * c2:i * NK + 2 * c2 + 2, t * LANES:t * LANES + wd]

    def exchange(src, dst, ss, rs):
        mine = pl.ds(pl.multiple_of(col * 8, 8), 8)
        for dlt in range(1, COLS):
            c2 = (col + dlt) % COLS
            send(src.at[c2], dst.at[:, mine, :], ss.at[dlt], rs.at[dlt], (c2, row))
        dst[:, mine, :] = src[col]

    def exchange_wait(dst, rs):
        for dlt in range(1, COLS):
            c2 = (col + COLS - dlt) % COLS
            arrive(dst.at[:, pl.ds(pl.multiple_of(c2 * 8, 8), 8), :], rs.at[dlt])

    def regroup(src, emit):
        for i in range(4):
            for jp in range(2):
                tiles = [src[t, pl.ds(2 * i + jp, 16, stride=8), :] for t, wd in lane_tiles(ab)]
                for a in range(va):
                    for t, wd in lane_tiles(nv):
                        first, shift = divmod(a * nv + t * LANES, LANES)
                        take = min(wd, LANES - shift)
                        val = tiles[first][:, shift:shift + take]
                        if take < wd:
                            val = jnp.concatenate([val, tiles[first + 1][:, :wd - take]], axis=1)
                        osc[2 * jp + t, pl.ds(a, 16, stride=va), 0:wd] = val
            cols = [osc[2 * jp + t, :, 0:wd] for jp in range(2) for t, wd in lane_tiles(nv)]
            emit(i, jnp.concatenate(cols, axis=1))

    def transpose_bf(val):
        return val.astype(F32).T.astype(BF16)

    def away(src_row, h):
        return jnp.logical_or(row != src_row, 2 * row + h != col)

    z_send(0)
    y_step(0, root)
    x_step()
    z_wait(0)
    y_step(0, rel != 0)
    x_rest(3)
    x_rest(1)
    x_rest(2)
    z_send(1)
    z_send(2)
    z_send(3)
    loads[1].wait()

    def flip_w(n, carry):
        cols = pl.ds(pl.multiple_of(n * LANES, LANES), LANES)
        w2[cols, :] = transpose_bf(wt[:, cols])
        return carry

    lax.fori_loop(0, NK * nv // LANES, flip_w, 0, unroll=3)
    vrow[...] = transpose_bf(vo_ref[...])
    y_forward(0)
    z_wait(1)
    y_step(1)

    for off in range(4):
        arrive(tc.at[2 * ((x + off) % 4) + 1 - k], sib_rs.at[off])
    for r2 in range(ROWS):
        piece = jnp.dot(vrow[...], tc[r2], preferred_element_type=F32).T
        xs[2 * r2] = piece[0:64]
        xs[2 * r2 + 1] = piece[64:]
    for s in (1, 2, 3):
        z2 = (z + s) % 4
        send(xs.at[pl.ds(4 * z2, 4)], xr.at[s], xa_ss.at[s], xa_rs.at[s], zdev(s))
    y_rest(0)
    loads[0].wait()
    ladder(0)
    z_wait(2)
    y_step(2)
    for s in (1, 2, 3):
        arrive(xr.at[s], xa_rs.at[s])
    xs2[...] = xs[pl.ds(4 * z, 4)] + xr[1] + xr[2] + xr[3]
    for s in (1, 2, 3):
        y2 = (y + s) % 4
        send(xs2.at[y2], xr2.at[s], xb_ss.at[s], xb_rs.at[s], (4 * z + y2, row))
    y_forward(1)
    mixed(0)
    pair_step(0)
    z_wait(3)
    y_step(3)
    y_forward(2)
    y_rest(1)
    ladder(1)

    loads[2].wait()
    for s in (1, 2, 3):
        arrive(xr2.at[s], xb_rs.at[s])
    iq[0:LANES, 0:LANES] = oo[...].astype(F32).T
    half = 64 * (col % 2)
    mine = iq[pl.ds(pl.multiple_of(half, 8), 64), 0:LANES]
    wp[...] = (mine + 0.5 * (xs2[y] + xr2[1] + xr2[2] + xr2[3])).astype(BF16)
    w_rows = pl.ds(pl.multiple_of(half, 16), 64)
    self_w = row == col // 2
    for dlt in range(COLS):
        cond = row != col // 2 if dlt == 0 else None
        send(wp, wtr.at[row, w_rows, :], w_ss.at[dlt], w_rs.at[row, col % 2], ((col + dlt) % COLS, col // 2), cond)

    @pl.when(self_w)
    def _():
        wtr[row, w_rows, :] = wp[...]

    pair_step(1)
    hop_step()
    mixed(1)
    y_forward(3)
    base[...] = d_ref[...].T
    split_rows(base, d_send)
    exchange(d_send, d_recv, d_ss, d_rs)
    y_rest(2)
    ladder(2)
    pair_step(2)
    fin_step(2)
    y_rest(3)
    ladder(3)
    mixed(2)
    pair_step(3)
    fin_step(3)

    for r2 in range(ROWS):
        for h in range(2):
            @pl.when(away(r2, h))
            def _():
                arrive(wtr.at[r2, pl.ds(64 * h, 64), :], w_rs.at[r2, h])
    own = vo_ref[...].astype(F32)
    for r2 in range(ROWS):
        own = own + jnp.dot(tc[r2], transpose_bf(wtr[r2]), preferred_element_type=F32)
    part[0, k] = part[0, k] + own
    mixed(3)

    for n in range(2):
        arrive(fin.at[n], fin_rs.at[n])
    base[...] = (part[0, k] + fin[0] + fin[1]).T
    split_rows(base, b_send)
    exchange(b_send, b_recv, b_ss, b_rs)

    exchange_wait(d_recv, d_rs)

    def emit_d(i, val):
        dmat[i * nv:(i + 1) * nv, :] = val

    regroup(d_recv, emit_d)
    for r2 in range(ROWS):
        @pl.when(r2 != row)
        def _():
            arrive(m_recv.at[r2], m_rs.at[r2])
        for h in range(2):
            @pl.when(away(r2, h))
            def _():
                arrive(i_recv.at[r2, h], i_rs.at[r2, h])
    for c2 in range(2):
        parts = []
        for i2 in range(2):
            for r2 in range(ROWS):
                iq[r2 * a2:(r2 + 1) * a2, 0:n_w] = i_recv[r2, c2, i2 * a2:(i2 + 1) * a2, :]
            parts.append(iq[...].T[0:n_w, 0:nv])
        acc[c2 * n_w:(c2 + 1) * n_w, :] = jnp.concatenate(parts, axis=1)
    for r2 in range(ROWS):
        for ip in range(2):
            for i2 in range(2):
                r0 = (2 * ip + i2) * nv + r2 * a2
                acc[r0:r0 + a2, :] = acc[r0:r0 + a2, :] + m_recv[r2, ip, i2 * a2:(i2 + 1) * a2, :]
    exchange_wait(b_recv, b_rs)

    def emit(i, val):
        rows = slice(i * nv, (i + 1) * nv)
        acc[rows, :] = (acc[rows, :] + val) / dmat[rows, :]

    regroup(b_recv, emit)
    out_ref[...] = acc[...].T
    for fn in finish:
        fn()


def solution(mesh):
    def local(t_blk, d_blk, vo_blk, v_blk, oo, w_blk):
        nv = w_blk.shape[0] // NK
        va = nv // 16
        ab = va * nv
        nt = len(lane_tiles(ab))
        nw = 2 * nv
        a2 = 2 * va
        nwt = len(lane_tiles(nw))
        lanes = LANES
        V = pltpu.VMEM
        S = lambda *s: pltpu.SemaphoreType.DMA(s)
        pad = lambda n: -(-n // lanes) * lanes
        scratch = [
            V((12, ab, BLK), BF16), V((4, 2 * ab, 256), BF16), V((ab, 2 * ab), BF16), V((nw, NK * nv), BF16),
            V((NK * nv, nw), BF16), V((lanes, lanes), BF16), V((lanes, ab), BF16),
            V((COLS, 64, lanes), F32), V((4, 4, 64, lanes), F32), V((4, 64, lanes), F32), V((4, 64, lanes), F32), V((64, lanes), BF16), V((ROWS, lanes, lanes), BF16),
            V((4, 2, ab, lanes), F32), V((4, ab, lanes), F32), V((2, ab // 2, lanes), F32), V((2, ab, lanes), F32),
            V((2 * a2, 256, lanes), F32), V((nwt, 8 * a2, lanes), F32),
            V((4, 2, 2, 2 * a2, nw), F32), V((ROWS, 2, 2 * a2, nw), F32), V((ROWS, 2, 2 * a2, nw), F32),
            V((pad(nv), pad(nw)), F32),
            V((lanes, ab), F32), V((COLS, nt, 8, lanes), F32), V((nt, 128, lanes), F32), V((COLS, nt, 8, lanes), F32), V((nt, 128, lanes), F32),
            V((4, nv, lanes), F32), V((4 * nv, nw), F32), V((4 * nv, nw), F32),
            S(3), S(4, 2), S(4, 2), S(4), S(4), S(4, 5), S(4, 2), S(4, 2, 3), S(4, 2, 2, 2), S(4, 2, 2),
            S(4), S(4), S(2), S(2), S(2), S(2),
            S(4), S(4), S(4), S(4), S(COLS), S(ROWS, 2), S(4, 2), S(8), S(4, 2, 2), S(ROWS, 2), S(COLS), S(COLS), S(COLS), S(COLS),
        ]
        vm = pl.BlockSpec(memory_space=pltpu.VMEM)
        hb = pl.BlockSpec(memory_space=pl.ANY)
        out = pl.pallas_call(
            functools.partial(sweep_kernel, nv),
            out_shape=jax.ShapeDtypeStruct((nw, 4 * nv), F32),
            in_specs=[vm, vm, vm, hb, hb, hb],
            out_specs=vm,
            scratch_shapes=scratch,
            compiler_params=pltpu.CompilerParams(
                collective_id=0, has_side_effects=True, vmem_limit_bytes=64 * 1024 * 1024 - 65536),
        )(t_blk.T, d_blk.T, vo_blk.T, v_blk.T, oo, w_blk.T)
        return out.T

    return jax.shard_map(
        local,
        mesh=mesh,
        in_specs=(P("row", "col"), P("row", "col"), P("row", "col"), P("row", "col"), P(None, None), P(None, "col")),
        out_specs=P("row", "col"),
        check_vma=False,
    )
```

```python
import functools
import jax
import jax.numpy as jnp
from jax import lax
from jax.experimental import pallas as pl
from jax.experimental.pallas import tpu as pltpu
from jax.sharding import PartitionSpec as P

MESH = pl.DeviceIdType.MESH
F32 = jnp.float32
BF16 = jnp.bfloat16
BLK = 128
NK = 32
ROWS, COLS = 8, 16
LANES = 128
K_STEP = 4


def lane_tiles(width):
    return [(t, min(LANES, width - LANES * t)) for t in range(-(-width // LANES))]


def dot_nt(lhs, rhs):
    return lax.dot_general(lhs, rhs, (((1,), (1,)), ((), ())), preferred_element_type=F32)


def sweep_kernel(
    nv,
    t_ref, d_ref, vo_ref, v_hbm, oo_hbm, w_hbm,
    out_ref,
    tc, tl, vv, wt, w2, oo, vrow,
    xs, xr, xs2, xr2, wp, wtr,
    part, pair, hop, fin,
    tf, acc_t, perm, near, m_send, m_recv, i_recv, iq,
    base, d_send, d_recv, b_send, b_recv, osc, dmat, acc,
    local_sem, x_ss, x_rs, sib_ss, sib_rs, z_ss, z_rs, y_ss, y_rs, f_ss,
    pair_ss, pair_rs, hop_ss, hop_rs, fin_ss, fin_rs,
    xa_ss, xa_rs, xb_ss, xb_rs, w_ss, w_rs, m_ss, m_rs, n_ss, n_rs, i_ss, i_rs, d_ss, d_rs, b_ss, b_rs,
):
    row = lax.axis_index("row")
    col = lax.axis_index("col")
    x, k = row // 2, row % 2
    z, y = col // 4, col % 4
    va = nv // 16
    ab = va * nv
    n_w = 2 * nv
    a2 = 2 * va
    cut = (va + 1) // 2 * nv
    halves = [(0, cut), (cut, ab - cut)]
    hrow = ab // 2
    sib = (col, 2 * x + 1 - k)
    finish = []

    def send(src, dst, ss, rs, dev, cond=None):
        cp = pltpu.make_async_remote_copy(
            src_ref=src, dst_ref=dst, send_sem=ss, recv_sem=rs, device_id=dev, device_id_type=MESH)
        if cond is None:
            cp.start()
            finish.append(cp.wait_send)
        else:
            @pl.when(cond)
            def _():
                cp.start()

            def done():
                @pl.when(cond)
                def _():
                    cp.wait_send()
            finish.append(done)

    def arrive(dst, rs):
        pltpu.make_async_remote_copy(
            src_ref=dst, dst_ref=dst, send_sem=rs, recv_sem=rs, device_id=(col, row), device_id_type=MESH
        ).wait_recv()

    loads = [
        pltpu.make_async_copy(v_hbm.at[pl.ds(0, hrow)], vv.at[0], local_sem.at[0]),
        pltpu.make_async_copy(v_hbm.at[pl.ds(hrow, hrow)], vv.at[1], local_sem.at[3]),
        pltpu.make_async_copy(w_hbm, wt, local_sem.at[1]),
        pltpu.make_async_copy(
            oo_hbm.at[pl.ds(pl.multiple_of(row * BLK, BLK), BLK), pl.ds(pl.multiple_of(col // 2 * LANES, LANES), LANES)],
            oo, local_sem.at[2]),
    ]
    load_v, load_v2, load_w, load_oo = loads
    for cp in loads:
        cp.start()

    barrier = pltpu.get_barrier_semaphore()
    for dlt in range(1, COLS):
        pl.semaphore_signal(barrier, inc=1, device_id=((col + dlt) % COLS, row), device_id_type=MESH)
    for dlt in range(1, 8):
        pl.semaphore_signal(barrier, inc=1, device_id=(col, (row + dlt) % 8), device_id_type=MESH)
    for r2 in range(ROWS):
        for h in range(2):
            pl.semaphore_signal(barrier, inc=1, device_id=(2 * row + h, r2), device_id_type=MESH)
    for s in (1, 3):
        pl.semaphore_signal(barrier, inc=1, device_id=(4 * z + (y + s) % 4, 2 * x + 1 - k), device_id_type=MESH)

    tc[row] = t_ref[...].astype(BF16)
    pl.semaphore_wait(barrier, 15 + 7 + 16 + 2)

    def xdev(s):
        return (col, 2 * ((x + s) % 4) + k)

    def zdev(s):
        return (4 * ((z + s) % 4) + y, row)

    def piece_of(blk, h):
        r0, rn = halves[h]
        return tc.at[blk, pl.ds(r0, rn), :]

    for h in range(2):
        src = piece_of(row, h)
        send(src, src, x_ss.at[0, h], x_rs.at[3, h], xdev(1))
        src = piece_of(row, 1 - h)
        send(src, src, x_ss.at[1, 1 - h], x_rs.at[1, 1 - h], xdev(3))
    send(tc.at[row], tc.at[row], sib_ss.at[0], sib_rs.at[0], sib)

    rel = (z - x + 4) % 4
    root = rel == 0
    kap = y // 2
    order = [0, 2, 1, 3]

    def x_step():
        for off, h, s, slot in ((3, 0, 1, 2), (1, 1, 3, 3)):
            xb = (x + off) % 4
            r0, rn = halves[h]
            piece = tc.at[2 * xb + k, pl.ds(r0, rn), :]
            arrive(piece, x_rs.at[off, h])
            send(piece, piece, x_ss.at[slot, h], x_rs.at[2, h], xdev(s))

    def x_rest(off):
        xb = (x + off) % 4
        todo = {3: (1,), 1: (0,), 2: (0, 1)}[off]
        for h in todo:
            r0, rn = halves[h]
            arrive(tc.at[2 * xb + k, pl.ds(r0, rn), :], x_rs.at[off, h])
        src = tc.at[2 * xb + k]
        send(src, src, sib_ss.at[off], sib_rs.at[off], sib)

    def z_send(o):
        off = order[o]
        xb = (x + off) % 4
        for h, (r0, rn) in enumerate(halves):
            src = tc.at[2 * xb + k, pl.ds(r0, rn), :]
            dst = tc.at[8 + xb, pl.ds(r0, rn), :]
            send(src, dst, z_ss.at[o, h], z_rs.at[o, h], zdev(1), root)
        for h, (r0, rn) in reversed(list(enumerate(halves))):
            src = tc.at[2 * xb + k, pl.ds(r0, rn), :]
            dst = tc.at[8 + xb, pl.ds(r0, rn), :]
            send(src, dst, z_ss.at[o, 2 + h], z_rs.at[o, h], zdev(3), root)

    def z_wait(o):
        off = order[o]
        xb = (x + off) % 4
        for h, (r0, rn) in enumerate(halves):
            dst = tc.at[8 + xb, pl.ds(r0, rn), :]

            @pl.when(rel != 0)
            def _():
                arrive(dst, z_rs.at[o, h])
            step = (1, 3)[h]
            send(dst, dst, z_ss.at[o, 4], z_rs.at[o, h], zdev(step), rel == step)

    def z_step(o):
        z_send(o)
        z_wait(o)

    def both(p, q):
        return q if p is None else jnp.logical_and(p, q)

    sel_root = jnp.where(root, 1, 0)

    def y_step(o, cond=None):
        off = order[o]
        xb = (x + off) % 4
        blk = sel_root * (2 * xb + k) + (1 - sel_root) * (8 + xb)
        lanes = pl.ds(pl.multiple_of(k * LANES, LANES), LANES)
        for h, (r0, rn) in enumerate(halves):
            for n, s in enumerate((1, 3)):
                g = abs(n - h)
                src = piece_of(blk, g)
                dst = tl.at[xb, pl.ds((y % 2) * ab + halves[g][0], halves[g][1]), lanes]
                send(src, dst, y_ss.at[o, g, n], y_rs.at[o, y % 2, k, g],
                     (4 * z + (y + s) % 4, 2 * x + kap), cond)
        for h, (r0, rn) in enumerate(halves):
            src = piece_of(blk, h)
            dst = tl.at[xb, pl.ds((y % 2) * ab + r0, rn), lanes]
            send(src, dst, y_ss.at[o, h, 2], y_rs.at[o, y % 2, k, h], sib, both(cond, kap != k))

        @pl.when(both(cond, kap == k))
        def _():
            tl[xb, pl.ds(pl.multiple_of((y % 2) * ab, 16), ab), lanes] = tc[blk]

    def y_piece(o, s, q, h):
        xb = (x + order[o]) % 4
        r0, rn = halves[h]
        return tl.at[xb, pl.ds(s * ab + r0, rn), pl.ds(pl.multiple_of(q * LANES, LANES), LANES)]

    def y_forward(o):
        for s in range(2):
            dist = (y - (2 * k + s) + 4) % 4
            for q in range(2):
                for h, step in ((0, 1), (1, 3)):
                    piece = y_piece(o, s, q, h)

                    @pl.when(dist == step)
                    def _():
                        arrive(piece, y_rs.at[o, s, q, h])
                    send(piece, piece, f_ss.at[o, s, q], y_rs.at[o, s, q, h],
                         (4 * z + (y + step) % 4, row), dist == step)

    def y_rest(o):
        for s in range(2):
            dist = (y - (2 * k + s) + 4) % 4
            for q in range(2):
                for h in range(2):
                    piece = y_piece(o, s, q, h)
                    other = (1, 3)[1 - h]
                    need = jnp.where(dist == other, 1, 0) + jnp.where(dist == 2, 1, 0) + (
                        jnp.where(dist == 0, 1, 0) * jnp.where(k == q, 0, 1))

                    @pl.when(need == 1)
                    def _():
                        arrive(piece, y_rs.at[o, s, q, h])

    def ladder(o):
        off = order[o]
        xb = (x + off) % 4

        def some_rows(n, carry):
            rows = pl.ds(pl.multiple_of(n * hrow, 8), hrow)
            prod = jnp.dot(vv[n], tl[xb], preferred_element_type=F32)
            part[o, 0, rows, :] = prod[:, :LANES]
            part[o, 1, rows, :] = prod[:, LANES:]
            return carry

        lax.fori_loop(0, 2, some_rows, 0)
        send(part.at[o, 1 - k], pair.at[o], pair_ss.at[o], pair_rs.at[o], sib)

    def pair_step(o):
        arrive(pair.at[o], pair_rs.at[o])
        part[o, k] = part[o, k] + pair[o]

    def hop_step():
        for n in range(2):
            send(part.at[1, k, pl.ds(n * hrow, hrow), :], hop.at[n], hop_ss.at[n], hop_rs.at[n], xdev(1 + 2 * n))

    def fin_step(o):
        n = o - 2
        arrive(hop.at[n], hop_rs.at[n])
        rows = pl.ds(n * hrow, hrow)
        part[o, k, rows, :] = part[o, k, rows, :] + hop[n]
        send(part.at[o, k], fin.at[n], fin_ss.at[n], fin_rs.at[n], xdev(order[o]))

    def mixed(o):
        off = order[o]
        xb = (x + off) % 4

        def turn(a, carry):
            blk = tl[xb, pl.ds(pl.multiple_of(a * nv, 16), nv), :]
            flip = dot_nt(perm[...], blk)
            for t, wd in lane_tiles(nv):
                tf[2 * a + t, :, 0:wd] = flip[:, t * LANES:t * LANES + wd]
            return carry

        lax.fori_loop(0, a2, turn, 0, unroll=2)

        def one(k0, carry):
            prod = 0.0
            for kk in [k0 * K_STEP + n for n in range(K_STEP)]:
                cols = []
                for t, wd in lane_tiles(nv):
                    rows = [tf[2 * a + t, pl.ds(pl.multiple_of(kk * 8, 8), 8), :] for a in range(a2)]
                    cols.append(jnp.concatenate(rows, axis=0)[:, :wd].astype(BF16))
                lhs = jnp.concatenate(cols, axis=1) if len(cols) > 1 else cols[0]
                prod = prod + jnp.dot(
                    lhs, w2[pl.ds(pl.multiple_of(kk * nv, 16), nv), :], preferred_element_type=F32)
            for t, wd in lane_tiles(n_w):
                acc_t[t, :, 0:wd] = acc_t[t, :, 0:wd] + prod[:, t * LANES:t * LANES + wd]
            return carry

        acc_t[...] = jnp.zeros_like(acc_t)
        lax.fori_loop(0, NK // K_STEP, one, 0)
        for q in range(2):
            for ip in range(2):
                for i2 in range(2):
                    for t, wd in lane_tiles(n_w):
                        m_send[o, q, ip, i2 * a2:(i2 + 1) * a2, t * LANES:t * LANES + wd] = acc_t[
                            t, pl.ds(q * 4 + ip * 2 + i2, a2, stride=8), :][:, :wd]
            r2 = 2 * xb + q
            own = r2 == row
            send(m_send.at[o, q], m_recv.at[row], m_ss.at[o, q], m_rs.at[row], (col, r2), jnp.logical_not(own))

            @pl.when(own)
            def _():
                m_recv[row] = m_send[o, q]

    def image_near(o):
        for q in range(2):
            for ip in range(2):
                c2 = 4 * ((x + order[o]) % 4) + 2 * q + ip
                own = c2 == col
                src = m_send.at[o, q, ip]
                send(src, near.at[col], n_ss.at[o, q, ip], n_rs.at[col], (c2, row), jnp.logical_not(own))

                @pl.when(own)
                def _():
                    near[col] = m_send[o, q, ip]

    def image_far():
        for r2 in range(ROWS):
            for c2 in (2 * r2, 2 * r2 + 1):
                @pl.when(col != c2)
                def _():
                    arrive(near.at[c2], n_rs.at[c2])
            own = row == r2
            send(near.at[pl.ds(2 * r2, 2)], i_recv.at[row], i_ss.at[r2], i_rs.at[row], (col, r2), jnp.logical_not(own))

            @pl.when(own)
            def _():
                i_recv[row] = near[pl.ds(2 * r2, 2)]

    def split_rows(src, dst):
        for c2 in range(COLS):
            for i in range(4):
                for t, wd in lane_tiles(ab):
                    dst[c2, t, 2 * i:2 * i + 2, 0:wd] = src[i * NK + 2 * c2:i * NK + 2 * c2 + 2, t * LANES:t * LANES + wd]

    def exchange(src, dst, ss, rs):
        mine = pl.ds(pl.multiple_of(col * 8, 8), 8)
        for dlt in range(1, COLS):
            c2 = (col + dlt) % COLS
            send(src.at[c2], dst.at[:, mine, :], ss.at[dlt], rs.at[dlt], (c2, row))
        dst[:, mine, :] = src[col]

    def exchange_wait(dst, rs):
        for dlt in range(1, COLS):
            c2 = (col + COLS - dlt) % COLS
            arrive(dst.at[:, pl.ds(pl.multiple_of(c2 * 8, 8), 8), :], rs.at[dlt])

    def regroup(src, emit):
        for i in range(4):
            for jp in range(2):
                tiles = [src[t, pl.ds(2 * i + jp, 16, stride=8), :] for t, wd in lane_tiles(ab)]
                for a in range(va):
                    for t, wd in lane_tiles(nv):
                        first, shift = divmod(a * nv + t * LANES, LANES)
                        take = min(wd, LANES - shift)
                        val = tiles[first][:, shift:shift + take]
                        if take < wd:
                            val = jnp.concatenate([val, tiles[first + 1][:, :wd - take]], axis=1)
                        osc[2 * jp + t, pl.ds(a, 16, stride=va), 0:wd] = val
            cols = [osc[2 * jp + t, :, 0:wd] for jp in range(2) for t, wd in lane_tiles(nv)]
            emit(i, jnp.concatenate(cols, axis=1))

    def transpose_bf(val):
        return val.astype(F32).T.astype(BF16)

    def away(src_row, h):
        return jnp.logical_or(row != src_row, 2 * row + h != col)

    z_send(0)
    y_step(0, root)
    x_step()
    z_wait(0)
    y_step(0, rel != 0)
    for off in (3, 1, 2):
        x_rest(off)
    for o in (1, 2, 3):
        z_send(o)
    load_w.wait()

    def flip_w(n, carry):
        cols = pl.ds(pl.multiple_of(n * LANES, LANES), LANES)
        w2[cols, :] = transpose_bf(wt[:, cols])
        return carry

    lax.fori_loop(0, NK * nv // LANES, flip_w, 0, unroll=3)
    vrow[...] = transpose_bf(vo_ref[...])
    r_id = lax.broadcasted_iota(jnp.int32, perm.shape, 0)
    c_id = lax.broadcasted_iota(jnp.int32, perm.shape, 1)
    perm[...] = jnp.where((r_id % 8) * NK + r_id // 8 == c_id, 1.0, 0.0).astype(BF16)
    y_forward(0)
    z_wait(1)
    y_step(1)

    for off in range(4):
        arrive(tc.at[2 * ((x + off) % 4) + 1 - k], sib_rs.at[off])
    for r2 in range(ROWS):
        piece = jnp.dot(vrow[...], tc[r2], preferred_element_type=F32).T
        xs[2 * r2] = piece[0:64]
        xs[2 * r2 + 1] = piece[64:]
    for s in (1, 2, 3):
        z2 = (z + s) % 4
        send(xs.at[pl.ds(4 * z2, 4)], xr.at[s], xa_ss.at[s], xa_rs.at[s], zdev(s))
    y_rest(0)
    load_v.wait()
    load_v2.wait()
    ladder(0)
    z_wait(2)
    y_step(2)
    y_forward(1)
    mixed(0)
    pair_step(0)
    z_wait(3)
    y_step(3)
    y_forward(2)
    y_rest(1)
    ladder(1)
    for s in (1, 2, 3):
        arrive(xr.at[s], xa_rs.at[s])
    xs2[...] = xs[pl.ds(4 * z, 4)] + xr[1] + xr[2] + xr[3]
    for s in (1, 2, 3):
        y2 = (y + s) % 4
        send(xs2.at[y2], xr2.at[s], xb_ss.at[s], xb_rs.at[s], (4 * z + y2, row))
    y_forward(3)
    pair_step(1)
    hop_step()
    y_rest(2)
    ladder(2)

    load_oo.wait()
    for s in (1, 2, 3):
        arrive(xr2.at[s], xb_rs.at[s])
    iq[0:LANES, 0:LANES] = oo[...].astype(F32).T
    half = 64 * (col % 2)
    mine = iq[pl.ds(pl.multiple_of(half, 8), 64), 0:LANES]
    wp[...] = (mine + 0.5 * (xs2[y] + xr2[1] + xr2[2] + xr2[3])).astype(BF16)
    w_rows = pl.ds(pl.multiple_of(half, 16), 64)
    for dlt in range(COLS):
        cond = row != col // 2 if dlt == 0 else None
        send(wp, wtr.at[row, w_rows, :], w_ss.at[dlt], w_rs.at[row, col % 2], ((col + dlt) % COLS, col // 2), cond)

    @pl.when(row == col // 2)
    def _():
        wtr[row, w_rows, :] = wp[...]

    image_near(0)
    mixed(1)
    image_near(1)
    y_rest(3)
    ladder(3)
    pair_step(2)
    fin_step(2)
    base[...] = d_ref[...].T
    split_rows(base, d_send)
    exchange(d_send, d_recv, d_ss, d_rs)
    pair_step(3)
    fin_step(3)
    mixed(2)
    image_near(2)
    mixed(3)
    image_near(3)

    for r2 in range(ROWS):
        for h in range(2):
            @pl.when(away(r2, h))
            def _():
                arrive(wtr.at[r2, pl.ds(64 * h, 64), :], w_rs.at[r2, h])
    own = vo_ref[...].astype(F32)
    for r2 in range(ROWS):
        own = own + jnp.dot(tc[r2], transpose_bf(wtr[r2]), preferred_element_type=F32)
    part[0, k] = part[0, k] + own
    image_far()

    for n in range(2):
        arrive(fin.at[n], fin_rs.at[n])
    base[...] = (part[0, k] + fin[0] + fin[1]).T
    split_rows(base, b_send)
    exchange(b_send, b_recv, b_ss, b_rs)

    exchange_wait(d_recv, d_rs)

    def emit_d(i, val):
        dmat[i * nv:(i + 1) * nv, :] = val

    regroup(d_recv, emit_d)
    for r2 in range(ROWS):
        @pl.when(r2 != row)
        def _():
            arrive(m_recv.at[r2], m_rs.at[r2])
            arrive(i_recv.at[r2], i_rs.at[r2])
    for c2 in range(2):
        parts = []
        for i2 in range(2):
            for r2 in range(ROWS):
                iq[r2 * a2:(r2 + 1) * a2, 0:n_w] = i_recv[r2, c2, i2 * a2:(i2 + 1) * a2, :]
            parts.append(iq[...].T[0:n_w, 0:nv])
        acc[c2 * n_w:(c2 + 1) * n_w, :] = jnp.concatenate(parts, axis=1)
    for r2 in range(ROWS):
        for ip in range(2):
            for i2 in range(2):
                r0 = (2 * ip + i2) * nv + r2 * a2
                acc[r0:r0 + a2, :] = acc[r0:r0 + a2, :] + m_recv[r2, ip, i2 * a2:(i2 + 1) * a2, :]
    exchange_wait(b_recv, b_rs)

    def emit(i, val):
        rows = slice(i * nv, (i + 1) * nv)
        acc[rows, :] = (acc[rows, :] + val) / dmat[rows, :]

    regroup(b_recv, emit)
    out_ref[...] = acc[...].T
    for fn in finish:
        fn()


def solution(mesh):
    def local(t_blk, d_blk, vo_blk, v_blk, oo, w_blk):
        nv = w_blk.shape[0] // NK
        va = nv // 16
        ab = va * nv
        nt = len(lane_tiles(ab))
        nw = 2 * nv
        a2 = 2 * va
        nwt = len(lane_tiles(nw))
        lanes = LANES
        V = pltpu.VMEM
        S = lambda *s: pltpu.SemaphoreType.DMA(s)
        pad = lambda n: -(-n // lanes) * lanes
        scratch = [
            V((12, ab, BLK), BF16), V((4, 2 * ab, 256), BF16), V((2, ab // 2, 2 * ab), BF16), V((nw, NK * nv), BF16),
            V((NK * nv, nw), BF16), V((lanes, lanes), BF16), V((lanes, ab), BF16),
            V((COLS, 64, lanes), F32), V((4, 4, 64, lanes), F32), V((4, 64, lanes), F32), V((4, 64, lanes), F32), V((64, lanes), BF16), V((ROWS, lanes, lanes), BF16),
            V((4, 2, ab, lanes), F32), V((4, ab, lanes), F32), V((2, ab // 2, lanes), F32), V((2, ab, lanes), F32),
            V((2 * a2, 256, lanes), F32), V((nwt, 8 * a2, lanes), F32),
            V((256, 256), BF16), V((COLS, 2 * a2, nw), F32), V((4, 2, 2, 2 * a2, nw), F32), V((ROWS, 2, 2 * a2, nw), F32), V((ROWS, 2, 2 * a2, nw), F32),
            V((pad(nv), pad(nw)), F32),
            V((lanes, ab), F32), V((COLS, nt, 8, lanes), F32), V((nt, 128, lanes), F32), V((COLS, nt, 8, lanes), F32), V((nt, 128, lanes), F32),
            V((4, nv, lanes), F32), V((4 * nv, nw), F32), V((4 * nv, nw), F32),
            S(4), S(4, 2), S(4, 2), S(4), S(4), S(4, 5), S(4, 2), S(4, 2, 3), S(4, 2, 2, 2), S(4, 2, 2),
            S(4), S(4), S(2), S(2), S(2), S(2),
            S(4), S(4), S(4), S(4), S(COLS), S(ROWS, 2), S(4, 2), S(8), S(4, 2, 2), S(COLS), S(ROWS), S(ROWS), S(COLS), S(COLS), S(COLS), S(COLS),
        ]
        vm = pl.BlockSpec(memory_space=pltpu.VMEM)
        hb = pl.BlockSpec(memory_space=pl.ANY)
        out = pl.pallas_call(
            functools.partial(sweep_kernel, nv),
            out_shape=jax.ShapeDtypeStruct((nw, 4 * nv), F32),
            in_specs=[vm, vm, vm, hb, hb, hb],
            out_specs=vm,
            scratch_shapes=scratch,
            compiler_params=pltpu.CompilerParams(
                collective_id=0, has_side_effects=True, vmem_limit_bytes=64 * 1024 * 1024 - 65536),
        )(t_blk.T, d_blk.T, vo_blk.T, v_blk.T, oo, w_blk.T)
        return out.T

    return jax.shard_map(
        local,
        mesh=mesh,
        in_specs=(P("row", "col"), P("row", "col"), P("row", "col"), P("row", "col"), P(None, None), P(None, "col")),
        out_specs=P("row", "col"),
        check_vma=False,
    )
```

```python
import functools
import jax
import jax.numpy as jnp
from jax import lax
from jax.experimental import pallas as pl
from jax.experimental.pallas import tpu as pltpu
from jax.sharding import PartitionSpec as P

MESH = pl.DeviceIdType.MESH
F32 = jnp.float32
BF16 = jnp.bfloat16
BLK = 128
NK = 32
ROWS, COLS = 8, 16
OTHERS = (1, 2, 3)
LANES = 128
K_STEP = 4


def lane_tiles(width):
    return [(t, min(LANES, width - LANES * t)) for t in range(-(-width // LANES))]


def piece_parts(nv, t, width, i2):
    a2 = nv // 8
    tall = -(-2 * a2 // 8) * 8
    if 4 * width > LANES:
        return [(t * tall + i2 * a2, a2, 0, 0)]
    return [(t * tall, a2 // 2, (2 * i2 + g) * width, g * (a2 // 2)) for g in range(2)]


def piece_rows(nv):
    a2 = nv // 8
    return sum(-(-(a2 // 2 if 4 * wd <= LANES else 2 * a2) // 8) * 8 for t, wd in lane_tiles(2 * nv))


def dot_nt(lhs, rhs):
    return lax.dot_general(lhs, rhs, (((1,), (1,)), ((), ())), preferred_element_type=F32)


def sweep_kernel(
    nv,
    t_ref, d_hbm, vo_hbm, v_hbm, oo_hbm, w_hbm,
    out_ref, d_ref, vo_ref,
    tc, tl, vv, wt, w2, oo, vrow,
    known, xs, xr, xs2, xr2, wp, wtr,
    part, pair, hop, fin,
    tf, acc_t, perm, near, m_send, m_recv, i_recv, iq,
    base, d_send, d_recv, b_send, b_recv, osc, dmat, acc,
    local_sem, x_ss, x_rs, sib_ss, sib_rs, z_ss, z_rs, y_ss, y_rs, f_ss,
    pair_ss, pair_rs, hop_ss, hop_rs, fin_ss, fin_rs,
    xa_ss, xa_rs, xb_ss, xb_rs, w_ss, w_rs, m_ss, m_rs, n_ss, n_rs, i_ss, i_rs, d_ss, d_rs, b_ss, b_rs,
):
    row = lax.axis_index("row")
    col = lax.axis_index("col")
    x, k = row // 2, row % 2
    z, y = col // 4, col % 4
    va = nv // 16
    ab = va * nv
    n_w = 2 * nv
    a2 = 2 * va
    cut = (va + 1) // 2 * nv
    halves = [(0, cut), (cut, ab - cut)]
    hrow = ab // 2
    sib = (col, 2 * x + 1 - k)
    finish = []

    def send(src, dst, ss, rs, dev, cond=None):
        cp = pltpu.make_async_remote_copy(
            src_ref=src, dst_ref=dst, send_sem=ss, recv_sem=rs, device_id=dev, device_id_type=MESH)
        if cond is None:
            cp.start()
            finish.append(cp.wait_send)
        else:
            @pl.when(cond)
            def _():
                cp.start()

            def done():
                @pl.when(cond)
                def _():
                    cp.wait_send()
            finish.append(done)

    def arrive(dst, rs):
        pltpu.make_async_remote_copy(
            src_ref=dst, dst_ref=dst, send_sem=rs, recv_sem=rs, device_id=(col, row), device_id_type=MESH
        ).wait_recv()

    loads = [
        pltpu.make_async_copy(v_hbm.at[pl.ds(0, hrow)], vv.at[0], local_sem.at[0]),
        pltpu.make_async_copy(v_hbm.at[pl.ds(hrow, hrow)], vv.at[1], local_sem.at[3]),
        pltpu.make_async_copy(w_hbm, wt, local_sem.at[1]),
        pltpu.make_async_copy(
            oo_hbm.at[pl.ds(pl.multiple_of(row * BLK, BLK), BLK), pl.ds(pl.multiple_of(col // 2 * LANES, LANES), LANES)],
            oo, local_sem.at[2]),
    ]
    loads += [pltpu.make_async_copy(vo_hbm, vo_ref, local_sem.at[4]), pltpu.make_async_copy(d_hbm, d_ref, local_sem.at[5])]
    load_v, load_v2, load_w, load_oo, load_vo, load_d = loads
    for cp in loads:
        cp.start()

    def xdev(s):
        return (col, 2 * ((x + s) % 4) + k)

    def zdev(s):
        return (4 * ((z + s) % 4) + y, row)

    def ydev(s, core):
        return (4 * z + (y + s) % 4, 2 * x + core)

    next_to = [sib] + [f(s) for f in (xdev, zdev) for s in (1, 3)] + [ydev(s, c) for s in (1, 3) for c in (k, 1 - k)]
    barrier = pltpu.get_barrier_semaphore()
    for dev in next_to:
        pl.semaphore_signal(barrier, inc=1, device_id=dev, device_id_type=MESH)

    def hello(n):
        for dev in next_to:
            pl.semaphore_signal(known.at[n], inc=1, device_id=dev, device_id_type=MESH)

    def heard(n):
        pl.semaphore_wait(known.at[n], len(next_to))

    tc[row] = t_ref[...].astype(BF16)
    pl.semaphore_wait(barrier, len(next_to))

    def piece_of(blk, h):
        r0, rn = halves[h]
        return tc.at[blk, pl.ds(r0, rn), :]

    for h in range(2):
        src = piece_of(row, h)
        send(src, src, x_ss.at[0, h], x_rs.at[3, h], xdev(1))
        src = piece_of(row, 1 - h)
        send(src, src, x_ss.at[1, 1 - h], x_rs.at[1, 1 - h], xdev(3))
    send(tc.at[row], tc.at[row], sib_ss.at[0], sib_rs.at[0], sib)

    rel = (z - x + 4) % 4
    root = rel == 0
    kap = y // 2
    order = [0, 2, 1, 3]

    def x_step():
        for off, h, s, slot in ((3, 0, 1, 2), (1, 1, 3, 3)):
            xb = (x + off) % 4
            r0, rn = halves[h]
            piece = tc.at[2 * xb + k, pl.ds(r0, rn), :]
            arrive(piece, x_rs.at[off, h])
            send(piece, piece, x_ss.at[slot, h], x_rs.at[2, h], xdev(s))

    def x_rest(off):
        xb = (x + off) % 4
        todo = {3: (1,), 1: (0,), 2: (0, 1)}[off]
        for h in todo:
            r0, rn = halves[h]
            arrive(tc.at[2 * xb + k, pl.ds(r0, rn), :], x_rs.at[off, h])
        src = tc.at[2 * xb + k]
        send(src, src, sib_ss.at[off], sib_rs.at[off], sib)

    def z_send(o):
        off = order[o]
        xb = (x + off) % 4
        for h, (r0, rn) in enumerate(halves):
            src = tc.at[2 * xb + k, pl.ds(r0, rn), :]
            dst = tc.at[8 + xb, pl.ds(r0, rn), :]
            send(src, dst, z_ss.at[o, h], z_rs.at[o, h], zdev(1), root)
        for h, (r0, rn) in reversed(list(enumerate(halves))):
            src = tc.at[2 * xb + k, pl.ds(r0, rn), :]
            dst = tc.at[8 + xb, pl.ds(r0, rn), :]
            send(src, dst, z_ss.at[o, 2 + h], z_rs.at[o, h], zdev(3), root)

    def z_wait(o):
        off = order[o]
        xb = (x + off) % 4
        for h, (r0, rn) in enumerate(halves):
            dst = tc.at[8 + xb, pl.ds(r0, rn), :]

            @pl.when(rel != 0)
            def _():
                arrive(dst, z_rs.at[o, h])
            step = (1, 3)[h]
            send(dst, dst, z_ss.at[o, 4], z_rs.at[o, h], zdev(step), rel == step)

    def z_step(o):
        z_send(o)
        z_wait(o)

    def both(p, q):
        return q if p is None else jnp.logical_and(p, q)

    sel_root = jnp.where(root, 1, 0)

    def y_step(o, cond=None):
        off = order[o]
        xb = (x + off) % 4
        blk = sel_root * (2 * xb + k) + (1 - sel_root) * (8 + xb)
        lanes = pl.ds(pl.multiple_of(k * LANES, LANES), LANES)
        for h, (r0, rn) in enumerate(halves):
            for n, s in enumerate((1, 3)):
                g = abs(n - h)
                src = piece_of(blk, g)
                dst = tl.at[xb, pl.ds((y % 2) * ab + halves[g][0], halves[g][1]), lanes]
                send(src, dst, y_ss.at[o, g, n], y_rs.at[o, y % 2, k, g],
                     (4 * z + (y + s) % 4, 2 * x + kap), cond)
        for h, (r0, rn) in enumerate(halves):
            src = piece_of(blk, h)
            dst = tl.at[xb, pl.ds((y % 2) * ab + r0, rn), lanes]
            send(src, dst, y_ss.at[o, h, 2], y_rs.at[o, y % 2, k, h], sib, both(cond, kap != k))

        @pl.when(both(cond, kap == k))
        def _():
            tl[xb, pl.ds(pl.multiple_of((y % 2) * ab, 16), ab), lanes] = tc[blk]

    def y_piece(o, s, q, h):
        xb = (x + order[o]) % 4
        r0, rn = halves[h]
        return tl.at[xb, pl.ds(s * ab + r0, rn), pl.ds(pl.multiple_of(q * LANES, LANES), LANES)]

    def y_forward(o):
        for s in range(2):
            dist = (y - (2 * k + s) + 4) % 4
            for q in range(2):
                for h, step in ((0, 1), (1, 3)):
                    piece = y_piece(o, s, q, h)

                    @pl.when(dist == step)
                    def _():
                        arrive(piece, y_rs.at[o, s, q, h])
                    send(piece, piece, f_ss.at[o, s, q], y_rs.at[o, s, q, h],
                         (4 * z + (y + step) % 4, row), dist == step)

    def y_rest(o):
        for s in range(2):
            dist = (y - (2 * k + s) + 4) % 4
            for q in range(2):
                for h in range(2):
                    piece = y_piece(o, s, q, h)
                    other = (1, 3)[1 - h]
                    need = jnp.where(dist == other, 1, 0) + jnp.where(dist == 2, 1, 0) + (
                        jnp.where(dist == 0, 1, 0) * jnp.where(k == q, 0, 1))

                    @pl.when(need == 1)
                    def _():
                        arrive(piece, y_rs.at[o, s, q, h])

    def ladder(o):
        off = order[o]
        xb = (x + off) % 4

        def some_rows(n, carry):
            rows = pl.ds(pl.multiple_of(n * hrow, 8), hrow)
            prod = jnp.dot(vv[n], tl[xb], preferred_element_type=F32)
            part[o, 0, rows, :] = prod[:, :LANES]
            part[o, 1, rows, :] = prod[:, LANES:]
            return carry

        lax.fori_loop(0, 2, some_rows, 0)
        send(part.at[o, 1 - k], pair.at[o], pair_ss.at[o], pair_rs.at[o], sib)

    def pair_step(o):
        arrive(pair.at[o], pair_rs.at[o])
        part[o, k] = part[o, k] + pair[o]

    def hop_step():
        for n in range(2):
            send(part.at[1, k, pl.ds(n * hrow, hrow), :], hop.at[n], hop_ss.at[n], hop_rs.at[n], xdev(1 + 2 * n))

    def fin_step(o):
        n = o - 2
        arrive(hop.at[n], hop_rs.at[n])
        rows = pl.ds(n * hrow, hrow)
        part[o, k, rows, :] = part[o, k, rows, :] + hop[n]
        send(part.at[o, k], fin.at[n], fin_ss.at[n], fin_rs.at[n], xdev(order[o]))

    def mixed(o):
        off = order[o]
        xb = (x + off) % 4

        def turn(a, carry):
            blk = tl[xb, pl.ds(pl.multiple_of(a * nv, 16), nv), :]
            flip = dot_nt(perm[...], blk)
            for t, wd in lane_tiles(nv):
                tf[2 * a + t, :, 0:wd] = flip[:, t * LANES:t * LANES + wd]
            return carry

        lax.fori_loop(0, a2, turn, 0, unroll=2)

        def one(k0, carry):
            prod = 0.0
            for kk in [k0 * K_STEP + n for n in range(K_STEP)]:
                cols = []
                for t, wd in lane_tiles(nv):
                    rows = [tf[2 * a + t, pl.ds(pl.multiple_of(kk * 8, 8), 8), :] for a in range(a2)]
                    cols.append(jnp.concatenate(rows, axis=0)[:, :wd].astype(BF16))
                lhs = jnp.concatenate(cols, axis=1) if len(cols) > 1 else cols[0]
                prod = prod + jnp.dot(
                    lhs, w2[pl.ds(pl.multiple_of(kk * nv, 16), nv), :], preferred_element_type=F32)
            for t, wd in lane_tiles(n_w):
                acc_t[t, :, 0:wd] = acc_t[t, :, 0:wd] + prod[:, t * LANES:t * LANES + wd]
            return carry

        acc_t[...] = jnp.zeros_like(acc_t)
        lax.fori_loop(0, NK // K_STEP, one, 0)
        for q in range(2):
            for ip in range(2):
                for i2 in range(2):
                    for t, wd in lane_tiles(n_w):
                        val = acc_t[t, pl.ds(q * 4 + ip * 2 + i2, a2, stride=8), :][:, :wd]
                        for r0, rn, c0, v0 in piece_parts(nv, t, wd, i2):
                            m_send[o, q, ip, r0:r0 + rn, c0:c0 + wd] = val[v0:v0 + rn]

    def mixed_far(o):
        xb = (x + order[o]) % 4
        for q in range(2):
            r2 = 2 * xb + q
            own = r2 == row
            send(m_send.at[o, q], m_recv.at[row], m_ss.at[o, q], m_rs.at[row], (col, r2), jnp.logical_not(own))

            @pl.when(own)
            def _():
                m_recv[row] = m_send[o, q]

    def unpack(src, i2):
        cols = []
        for t, wd in lane_tiles(n_w):
            rows = [src[r0:r0 + rn, c0:c0 + wd] for r0, rn, c0, v0 in piece_parts(nv, t, wd, i2)]
            cols.append(jnp.concatenate(rows, axis=0) if len(rows) > 1 else rows[0])
        return jnp.concatenate(cols, axis=1) if len(cols) > 1 else cols[0]

    def image_near(o):
        for q in range(2):
            for ip in range(2):
                c2 = 4 * ((x + order[o]) % 4) + 2 * q + ip
                own = c2 == col
                src = m_send.at[o, q, ip]
                send(src, near.at[col], n_ss.at[o, q, ip], n_rs.at[col], (c2, row), jnp.logical_not(own))

                @pl.when(own)
                def _():
                    near[col] = m_send[o, q, ip]

    def image_far():
        for r2 in range(ROWS):
            for c2 in (2 * r2, 2 * r2 + 1):
                @pl.when(col != c2)
                def _():
                    arrive(near.at[c2], n_rs.at[c2])
            own = row == r2
            send(near.at[pl.ds(2 * r2, 2)], i_recv.at[row], i_ss.at[r2], i_rs.at[row], (col, r2), jnp.logical_not(own))

            @pl.when(own)
            def _():
                i_recv[row] = near[pl.ds(2 * r2, 2)]

    def split_rows(src, dst):
        for c2 in range(COLS):
            for i in range(4):
                for t, wd in lane_tiles(ab):
                    dst[c2, t, 2 * i:2 * i + 2, 0:wd] = src[i * NK + 2 * c2:i * NK + 2 * c2 + 2, t * LANES:t * LANES + wd]

    def exchange(src, dst, ss, rs):
        mine = pl.ds(pl.multiple_of(col * 8, 8), 8)
        for dlt in range(1, COLS):
            c2 = (col + dlt) % COLS
            send(src.at[c2], dst.at[:, mine, :], ss.at[dlt], rs.at[dlt], (c2, row))
        dst[:, mine, :] = src[col]

    def exchange_wait(dst, rs):
        for dlt in range(1, COLS):
            c2 = (col + COLS - dlt) % COLS
            arrive(dst.at[:, pl.ds(pl.multiple_of(c2 * 8, 8), 8), :], rs.at[dlt])

    def regroup(src, emit):
        for i in range(4):
            for jp in range(2):
                tiles = [src[t, pl.ds(2 * i + jp, 16, stride=8), :] for t, wd in lane_tiles(ab)]
                for a in range(va):
                    for t, wd in lane_tiles(nv):
                        first, shift = divmod(a * nv + t * LANES, LANES)
                        take = min(wd, LANES - shift)
                        val = tiles[first][:, shift:shift + take]
                        if take < wd:
                            val = jnp.concatenate([val, tiles[first + 1][:, :wd - take]], axis=1)
                        osc[2 * jp + t, pl.ds(a, 16, stride=va), 0:wd] = val
            cols = [osc[2 * jp + t, :, 0:wd] for jp in range(2) for t, wd in lane_tiles(nv)]
            emit(i, jnp.concatenate(cols, axis=1))

    def transpose_bf(val):
        return val.astype(F32).T.astype(BF16)

    def away(src_row, h):
        return jnp.logical_or(row != src_row, 2 * row + h != col)

    z_send(0)
    y_step(0, root)
    hello(0)
    x_step()
    z_wait(0)
    y_step(0, rel != 0)
    heard(0)
    hello(1)
    for off in (3, 1, 2):
        x_rest(off)
    for o in OTHERS:
        z_send(o)
    heard(1)
    hello(2)
    load_w.wait()

    def flip_w(n, carry):
        cols = pl.ds(pl.multiple_of(n * LANES, LANES), LANES)
        w2[cols, :] = transpose_bf(wt[:, cols])
        return carry

    lax.fori_loop(0, NK * nv // LANES, flip_w, 0, unroll=3)
    load_vo.wait()
    vrow[...] = transpose_bf(vo_ref[...])
    r_id = lax.broadcasted_iota(jnp.int32, perm.shape, 0)
    c_id = lax.broadcasted_iota(jnp.int32, perm.shape, 1)
    perm[...] = jnp.where((r_id % 8) * NK + r_id // 8 == c_id, 1.0, 0.0).astype(BF16)
    heard(2)
    hello(3)
    y_forward(0)
    z_wait(1)
    y_step(1)

    for off in range(4):
        arrive(tc.at[2 * ((x + off) % 4) + 1 - k], sib_rs.at[off])
    for r2 in range(ROWS):
        piece = jnp.dot(vrow[...], tc[r2], preferred_element_type=F32).T
        xs[2 * r2] = piece[0:64]
        xs[2 * r2 + 1] = piece[64:]
    for s in OTHERS:
        z2 = (z + s) % 4
        send(xs.at[pl.ds(4 * z2, 4)], xr.at[s], xa_ss.at[s], xa_rs.at[s], zdev(s))
    y_rest(0)
    load_v.wait()
    load_v2.wait()
    ladder(0)
    z_wait(2)
    y_step(2)
    heard(3)
    hello(4)
    y_forward(1)
    mixed(0)
    mixed_far(0)
    pair_step(0)
    z_wait(3)
    y_step(3)
    y_forward(2)
    y_rest(1)
    ladder(1)
    for s in OTHERS:
        arrive(xr.at[s], xa_rs.at[s])
    xs2[...] = xs[pl.ds(4 * z, 4)] + xr[1] + xr[2] + xr[3]
    for s in OTHERS:
        y2 = (y + s) % 4
        send(xs2.at[y2], xr2.at[s], xb_ss.at[s], xb_rs.at[s], (4 * z + y2, row))
    mixed(1)
    pair_step(1)
    hop_step()
    mixed_far(1)
    y_forward(3)
    y_rest(2)
    ladder(2)

    load_oo.wait()
    heard(4)
    for s in OTHERS:
        arrive(xr2.at[s], xb_rs.at[s])
    iq[0:LANES, 0:LANES] = oo[...].astype(F32).T
    half = 64 * (col % 2)
    mine = iq[pl.ds(pl.multiple_of(half, 8), 64), 0:LANES]
    wp[...] = (mine + 0.5 * (xs2[y] + xr2[1] + xr2[2] + xr2[3])).astype(BF16)
    w_rows = pl.ds(pl.multiple_of(half, 16), 64)
    for dlt in range(COLS):
        cond = row != col // 2 if dlt == 0 else None
        send(wp, wtr.at[row, w_rows, :], w_ss.at[dlt], w_rs.at[row, col % 2], ((col + dlt) % COLS, col // 2), cond)

    @pl.when(row == col // 2)
    def _():
        wtr[row, w_rows, :] = wp[...]

    image_near(0)
    image_near(1)
    y_rest(3)
    ladder(3)
    pair_step(2)
    fin_step(2)
    load_d.wait()
    base[...] = d_ref[...].T
    split_rows(base, d_send)
    exchange(d_send, d_recv, d_ss, d_rs)
    pair_step(3)
    fin_step(3)
    mixed(2)
    image_near(2)
    mixed_far(2)
    mixed(3)
    image_near(3)
    mixed_far(3)

    for r2 in range(ROWS):
        for h in range(2):
            @pl.when(away(r2, h))
            def _():
                arrive(wtr.at[r2, pl.ds(64 * h, 64), :], w_rs.at[r2, h])
    own = vo_ref[...].astype(F32)
    for r2 in range(ROWS):
        own = own + jnp.dot(tc[r2], transpose_bf(wtr[r2]), preferred_element_type=F32)
    part[0, k] = part[0, k] + own
    image_far()

    for n in range(2):
        arrive(fin.at[n], fin_rs.at[n])
    base[...] = (part[0, k] + fin[0] + fin[1]).T
    split_rows(base, b_send)
    exchange(b_send, b_recv, b_ss, b_rs)

    exchange_wait(d_recv, d_rs)

    def emit_d(i, val):
        dmat[i * nv:(i + 1) * nv, :] = val

    regroup(d_recv, emit_d)
    for r2 in range(ROWS):
        @pl.when(r2 != row)
        def _():
            arrive(m_recv.at[r2], m_rs.at[r2])
        for ip in range(2):
            for i2 in range(2):
                r0 = (2 * ip + i2) * nv + r2 * a2
                acc[r0:r0 + a2, :] = unpack(m_recv.at[r2, ip], i2)
    for r2 in range(ROWS):
        @pl.when(r2 != row)
        def _():
            arrive(i_recv.at[r2], i_rs.at[r2])
    for c2 in range(2):
        parts = []
        for i2 in range(2):
            for r2 in range(ROWS):
                iq[r2 * a2:(r2 + 1) * a2, 0:n_w] = unpack(i_recv.at[r2, c2], i2)
            parts.append(iq[...].T[0:n_w, 0:nv])
        rows = slice(c2 * n_w, (c2 + 1) * n_w)
        acc[rows, :] = acc[rows, :] + jnp.concatenate(parts, axis=1)
    exchange_wait(b_recv, b_rs)

    def emit(i, val):
        rows = slice(i * nv, (i + 1) * nv)
        acc[rows, :] = (acc[rows, :] + val) / dmat[rows, :]

    regroup(b_recv, emit)
    out_ref[...] = acc[...].T
    for fn in finish:
        fn()


def solution(mesh):
    def local(t_blk, d_blk, vo_blk, v_blk, oo, w_blk):
        nv = w_blk.shape[0] // NK
        va = nv // 16
        ab = va * nv
        nt = len(lane_tiles(ab))
        nw = 2 * nv
        a2 = 2 * va
        nwt = len(lane_tiles(nw))
        pr = piece_rows(nv)
        lanes = LANES
        V = pltpu.VMEM
        S = lambda *s: pltpu.SemaphoreType.DMA(s)
        pad = lambda n: -(-n // lanes) * lanes
        scratch = [
            V((ab, BLK), F32), V((ab, BLK), BF16),
            V((12, ab, BLK), BF16), V((4, 2 * ab, 256), BF16), V((2, ab // 2, 2 * ab), BF16), V((nw, NK * nv), BF16),
            V((NK * nv, nw), BF16), V((lanes, lanes), BF16), V((lanes, ab), BF16),
            pltpu.SemaphoreType.REGULAR((5,)), V((COLS, 64, lanes), F32), V((4, 4, 64, lanes), F32), V((4, 64, lanes), F32), V((4, 64, lanes), F32), V((64, lanes), BF16), V((ROWS, lanes, lanes), BF16),
            V((4, 2, ab, lanes), F32), V((4, ab, lanes), F32), V((2, ab // 2, lanes), F32), V((2, ab, lanes), F32),
            V((2 * a2, 256, lanes), F32), V((nwt, 8 * a2, lanes), F32),
            V((256, 256), BF16), V((COLS, pr, lanes), F32), V((4, 2, 2, pr, lanes), F32), V((ROWS, 2, pr, lanes), F32), V((ROWS, 2, pr, lanes), F32),
            V((pad(nv), pad(nw)), F32),
            V((lanes, ab), F32), V((COLS, nt, 8, lanes), F32), V((nt, 128, lanes), F32), V((COLS, nt, 8, lanes), F32), V((nt, 128, lanes), F32),
            V((4, nv, lanes), F32), V((4 * nv, nw), F32), V((4 * nv, nw), F32),
            S(6), S(4, 2), S(4, 2), S(4), S(4), S(4, 5), S(4, 2), S(4, 2, 3), S(4, 2, 2, 2), S(4, 2, 2),
            S(4), S(4), S(2), S(2), S(2), S(2),
            S(4), S(4), S(4), S(4), S(COLS), S(ROWS, 2), S(4, 2), S(8), S(4, 2, 2), S(COLS), S(ROWS), S(ROWS), S(COLS), S(COLS), S(COLS), S(COLS),
        ]
        vm = pl.BlockSpec(memory_space=pltpu.VMEM)
        hb = pl.BlockSpec(memory_space=pl.ANY)
        out = pl.pallas_call(
            functools.partial(sweep_kernel, nv),
            out_shape=jax.ShapeDtypeStruct((nw, 4 * nv), F32),
            in_specs=[vm] + [hb] * 5,
            out_specs=vm,
            scratch_shapes=scratch,
            compiler_params=pltpu.CompilerParams(
                collective_id=0, has_side_effects=True, vmem_limit_bytes=64 * 1024 * 1024 - 65536),
        )(t_blk.T, d_blk.T, vo_blk.T, v_blk.T, oo, w_blk.T)
        return out.T

    return jax.shard_map(
        local,
        mesh=mesh,
        in_specs=(P("row", "col"), P("row", "col"), P("row", "col"), P("row", "col"), P(None, None), P(None, "col")),
        out_specs=P("row", "col"),
        check_vma=False,
    )
```
